256 devices in a mesh: tp: 16 (over y_hi, z), dp: 16 (over y_lo, x, core).
Axes of the slice: x: 4, y: 4 (y_hi: 2, y_lo: 2; y = y_hi * 2 + y_lo), z: 8, core: 2. Of those that a mesh axis runs over, the one named last changes fastest.
Arguments:
- tokens: bfloat16 [6144, 4096], P(('dp', 'tp')), may hold values from -24 to 24
- hidden_grad: bfloat16 [6144, 14336], P('dp', 'tp'), may hold values from -0.59765625 to 0.59765625
- gate_value: bfloat16 [6144, 14336], P('dp', 'tp'), may hold values from -6 to 6
- up_value: bfloat16 [6144, 14336], P('dp', 'tp'), may hold values from -6 to 6
- gate_weight: bfloat16 [4096, 14336], P('dp', 'tp'), may hold values from -0.09375 to 0.09375
- up_weight: bfloat16 [4096, 14336], P('dp', 'tp'), may hold values from -0.09375 to 0.09375
Outputs:
- input_grad: bfloat16 [6144, 4096], P(('dp', 'tp'))
- gate_grad: bfloat16 [4096, 14336], P('dp', 'tp')
- up_grad: bfloat16 [4096, 14336], P('dp', 'tp')
The draws below stay inside these ranges and needn't reach their ends.
All inputs are finite; a program needn't handle non-finite values.
Results may differ from the reference program's by a relative error of at most 0.018.
Values may be sent and summed in bfloat16 or wider, within the bound.
No kernel may reach another device: no remote copies, remote signals or barrier semaphores. Data moves between devices by JAX's collectives and lax.ppermute only.
A program may use at most 128 MiB of HBM per device.

```python
import jax
import jax.numpy as jnp
from jax import lax

D = 4096
FF = 14336
TOK_DEV = 24
TOKENS = 6144
N_TP = 16
N_DP = 16


def spiked(drawn, key, source, target, shards_of, factor):
    owner, partner = [(jnp.arange(drawn.shape[axis_at]) // (drawn.shape[axis_at] // shards_of)).reshape([-1 if axis == axis_at else 1 for axis in range(drawn.ndim)]) for axis_at in (source, target)]
    chosen = jax.random.permutation(key, shards_of)[partner]
    strong = (owner == chosen) | (owner == (partner + shards_of // 2) % shards_of)
    return jnp.where(strong, factor * drawn, drawn)


def block_levels(own_key, shape, pieces, least, high):
    factor_of = 1.0
    for axis_at, shards_of in pieces:
        heights = jax.random.uniform(jax.random.fold_in(jax.random.fold_in(own_key, 6), axis_at), (shards_of,), jnp.float32, least / len(pieces), high / len(pieces))
        factor_of = factor_of * jnp.repeat(jnp.exp(heights), shape[axis_at] // shards_of).reshape((-1,) + (1,) * (len(shape) - 1 - axis_at))
    return factor_of


def normal_values(key, extent, deviation, bound, shards=(), held_as=jnp.bfloat16):
    entries = deviation * jax.random.normal(key, extent, jnp.float32)
    if shards:
        entries = entries * block_levels(key, extent, shards, -0.22, 0.18)
    return jnp.clip(entries, -bound, bound).astype(held_as)


def noise_with(key, extent, scale, reach, pieces, heavy, held_as=jnp.bfloat16):
    array = scale * jax.random.normal(key, extent, jnp.float32)
    if pieces:
        array = array * block_levels(key, extent, pieces, -0.22, 0.18)
    return jnp.clip(spiked(array, jax.random.fold_in(key, 3), *heavy), -reach, reach).astype(held_as)


def setup_inputs(seed: int = 0) -> dict:
    keys = jax.random.split(jax.random.key(seed), 7)
    tokens = noise_with(keys[0], (TOKENS, D), 1.0, 24.0, ((0, 256),), (0, 1, 256, 6.0))
    hidden_grad = normal_values(keys[1], (TOKENS, FF), 0.1, 0.59765625, ((0, 16), (1, 16)))
    gate_value = normal_values(keys[2], (TOKENS, FF), 1.0, 6.0, ((0, 16), (1, 16)))
    up_value = normal_values(keys[3], (TOKENS, FF), 1.0, 6.0, ((0, 16), (1, 16)))
    gate_weight = normal_values(keys[4], (D, FF), D ** -0.5, 0.09375, ((0, 16), (1, 16)))
    up_weight = normal_values(keys[5], (D, FF), D ** -0.5, 0.09375, ((0, 16), (1, 16)))
    return dict(tokens=tokens, hidden_grad=hidden_grad, gate_value=gate_value, up_value=up_value, gate_weight=gate_weight, up_weight=up_weight)


def reference(tokens, hidden_grad, gate_value, up_value, gate_weight, up_weight):
    gate_float = gate_value.astype(jnp.float32)
    up_float = up_value.astype(jnp.float32)
    logistic = jax.nn.sigmoid(gate_float)
    upstream = hidden_grad.astype(jnp.float32)
    d_gate = (upstream * up_float * logistic * (1.0 + gate_float * (1.0 - logistic))).astype(jnp.bfloat16)
    d_up = (upstream * gate_float * logistic).astype(jnp.bfloat16)
    input_grad = (jnp.dot(d_gate, gate_weight.T, preferred_element_type=jnp.float32)
                  + jnp.dot(d_up, up_weight.T, preferred_element_type=jnp.float32)).astype(jnp.bfloat16)
    group_rows = TOK_DEV * N_TP
    contract = (((0,), (0,)), ((), ()))

    def per_group(carried, group_index):
        first_row = (group_index * group_rows).astype(jnp.int32)
        block = lax.dynamic_slice_in_dim(tokens, first_row, group_rows, 0)
        gate_rows = lax.dynamic_slice_in_dim(d_gate, first_row, group_rows, 0)
        up_rows = lax.dynamic_slice_in_dim(d_up, first_row, group_rows, 0)
        gate_part = lax.dot_general(block, gate_rows, contract, preferred_element_type=jnp.float32).astype(jnp.bfloat16)
        up_part = lax.dot_general(block, up_rows, contract, preferred_element_type=jnp.float32).astype(jnp.bfloat16)
        gate_part, up_part = lax.optimization_barrier((gate_part, up_part))
        return (carried[0] + gate_part.astype(jnp.float32), carried[1] + up_part.astype(jnp.float32)), None

    empty = jnp.zeros((D, FF), jnp.float32)
    summed, unused = lax.scan(per_group, (empty, empty), jnp.arange(N_DP, dtype=jnp.int32))
    return input_grad, summed[0].astype(jnp.bfloat16), summed[1].astype(jnp.bfloat16)
```

```python
import jax
import jax.numpy as jnp
from jax import lax
from jax.experimental import pallas as pl
from jax.experimental.pallas import tpu as pltpu
from jax.sharding import Mesh
from jax.sharding import PartitionSpec as P

AXES = ("yh", "z", "yl", "x", "c")
BF = jnp.bfloat16
F32 = jnp.float32
VMEM = pltpu.VMEM


def shift(v, axis, by):
    n = lax.axis_size(axis)
    return lax.ppermute(v, axis, [(i, (i + by) % n) for i in range(n)])


def swap(v, m):
    return lax.ppermute(v, ("yl", "c"), [(i, i ^ m) for i in range(4)])


def hidden_kernel(h_ref, g_ref, u_ref, dg_ref, du_ref):
    yh, z = lax.axis_index("yh"), lax.axis_index("z")
    nz = dg_ref.shape[0]
    for j in range(nz):
        for a in range(2):
            row = lax.rem(yh + a, 2) * nz + lax.rem(z + j, nz)
            h = h_ref[row].astype(F32)
            g = g_ref[row].astype(F32)
            u = u_ref[row].astype(F32)
            s = jax.nn.sigmoid(g)
            hs = h * s
            dg_ref[j, a] = (hs * u * (1.0 + g * (1.0 - s))).astype(BF)
            du_ref[j, a] = (hs * g).astype(BF)


def hidden_grads(h, g, u):
    n_yh, nz = lax.axis_size("yh"), lax.axis_size("z")
    rows, width = h.shape
    part = rows // (n_yh * nz)
    shape = jax.ShapeDtypeStruct((nz, n_yh, part, width), BF)
    view = [a.reshape(n_yh * nz, part, width) for a in (h, g, u)]
    dg, du = pl.pallas_call(
        hidden_kernel,
        out_shape=(shape, shape),
        in_specs=[pl.BlockSpec(memory_space=VMEM)] * 3,
        out_specs=[pl.BlockSpec(memory_space=VMEM)] * 2,
        name="hidden",
    )(*view)
    return dg.reshape(rows, width), du.reshape(rows, width)


X_ORDER = (2, 1, 3, 0)


def token_kernel(t_ref, o_ref):
    yl, x, c = lax.axis_index("yl"), lax.axis_index("x"), lax.axis_index("c")
    for m in range(4):
        yt = lax.bitwise_xor(yl, m // 2)
        ct = lax.bitwise_xor(c, m % 2)
        for j, rel in enumerate(X_ORDER):
            block = yt * 8 + lax.rem(x + rel, 4) * 2 + ct
            col = pl.multiple_of(block * 256, 256)
            o_ref[m, :, j * 256 : (j + 1) * 256] = t_ref[:, pl.ds(col, 256)]


def token_parts(t):
    rows, width = t.shape
    return pl.pallas_call(
        token_kernel,
        out_shape=jax.ShapeDtypeStruct((4, rows, width // 4), BF),
        in_specs=[pl.BlockSpec(memory_space=VMEM)],
        out_specs=pl.BlockSpec(memory_space=VMEM),
        name="token_parts",
    )(t)


def gather_z(b):
    out = [b] + [None] * 7
    left = right = b
    for k in range(1, 4):
        left = shift(left, "z", 1)
        right = shift(right, "z", -1)
        out[8 - k], out[k] = left, right
    half0 = shift(left[:2], "z", 1)
    half1 = shift(right[2:], "z", -1)
    out[4] = jnp.concatenate([half0, half1], axis=0)
    return out


def scatter_z(p):
    f = [a.astype(F32) for a in p]
    up = shift(p[0][4], "z", 1)
    down = shift(p[1][4], "z", -1)
    up = jnp.stack([f[0][3] + up.astype(F32), f[1][3]]).astype(BF)
    down = jnp.stack([f[0][5], f[1][5] + down.astype(F32)]).astype(BF)
    both = lambda j: jnp.stack([f[0][j], f[1][j]])
    for k in (2, 1):
        up = shift(up, "z", 1)
        down = shift(down, "z", -1)
        up = (both(k) + up.astype(F32)).astype(BF)
        down = (both(8 - k) + down.astype(F32)).astype(BF)
    up = shift(up, "z", 1)
    down = shift(down, "z", -1)
    return both(0) + up.astype(F32) + down.astype(F32)


def finish_kernel(s_ref, o_ref):
    yh, yl = lax.axis_index("yh"), lax.axis_index("yl")
    x, c = lax.axis_index("x"), lax.axis_index("c")
    for m in range(4):
        at = lax.bitwise_xor(yl, m // 2) * 2 + lax.bitwise_xor(c, m % 2)
        for a in range(2):
            yt = lax.bitwise_xor(yh, a)
            for j, rel in enumerate(X_ORDER):
                col = pl.multiple_of(lax.rem(x + rel, 4) * 256, 256)
                o_ref[yt * 4 + at, :, pl.ds(col, 256)] = s_ref[m, a, :, j * 256 : (j + 1) * 256]


def finish(s):
    return pl.pallas_call(
        finish_kernel,
        out_shape=jax.ShapeDtypeStruct((8, *s.shape[2:]), BF),
        in_specs=[pl.BlockSpec(memory_space=VMEM)],
        out_specs=pl.BlockSpec(memory_space=VMEM),
        name="finish",
    )(s)


def on_device(tokens, hidden_grad, gate_value, up_value, gate_weight, up_weight):
    weights = []
    gw, uw = gate_weight, up_weight
    g_left, g_right = shift(gw, "x", 1), shift(gw, "x", -1)
    u_left, u_right = shift(uw, "x", 1), shift(uw, "x", -1)
    g_far = shift(g_left, "x", 1)
    u_far = shift(u_right, "x", -1)
    gate_rows = (g_far, g_right, g_left, gw)
    up_rows = (u_far, u_right, u_left, uw)

    dg0, du0 = hidden_grads(hidden_grad, gate_value, up_value)
    dg2, du2 = swap(dg0, 2), swap(du0, 2)
    dg1, du1 = swap(dg0, 1), swap(du0, 1)
    dg3, du3 = swap(dg2, 1), swap(du2, 1)
    dg, du = (dg0, dg1, dg2, dg3), (du0, du1, du2, du3)

    parts = token_parts(tokens)
    block = jnp.stack([parts[0]] + [swap(parts[m], m) for m in (1, 2, 3)])
    other = shift(block, "yh", 1)
    mine, theirs = gather_z(block), gather_z(other)
    rows = tokens.shape[0]
    token_rows = jnp.stack([p for j in range(8) for p in (mine[j], theirs[j])], axis=1)
    token_rows = token_rows.reshape(4 * 16 * rows, -1)

    across = (((1,), (1,)), ((), ()))
    gate_mat = jnp.concatenate(gate_rows, axis=0)
    up_mat = jnp.concatenate(up_rows, axis=0)
    sums = []
    for first in (0, 2):
        p = []
        for m in (first, first + 1):
            v = lax.dot_general(dg[m], gate_mat, across, preferred_element_type=F32)
            v = v + lax.dot_general(du[m], up_mat, across, preferred_element_type=F32)
            p.append(v.astype(BF).reshape(8, 2 * rows, -1))
        sums.append(scatter_z(p))
    total = jnp.concatenate(sums, axis=0).astype(BF)
    ready = finish(total.reshape(4, 2, rows, -1))
    got = lax.all_to_all(ready, ("yh", "yl", "c"), 0, 0)
    got = got.reshape(2, 2, 2, rows, 4, 256).astype(F32)
    input_grad = (got[0] + got[1]).astype(BF)
    input_grad = input_grad.transpose(2, 0, 3, 1, 4).reshape(tokens.shape)

    contract = (((0,), (0,)), ((), ()))
    dg_all = jnp.concatenate(dg, axis=0)
    du_all = jnp.concatenate(du, axis=0)

    def part(d, j):
        cols = token_rows[:, j * 256 : (j + 1) * 256]
        return lax.dot_general(cols, d, contract, preferred_element_type=F32)

    g_two = shift(part(dg_all, 0).astype(BF), "x", 1)
    u_two = shift(part(du_all, 0).astype(BF), "x", -1)
    u_up = shift(part(du_all, 1).astype(BF), "x", 1)
    g_down = shift(part(dg_all, 2).astype(BF), "x", -1)
    g_up = shift((part(dg_all, 1) + g_two.astype(F32)).astype(BF), "x", 1)
    u_down = shift((part(du_all, 2) + u_two.astype(F32)).astype(BF), "x", -1)
    gate_grad = part(dg_all, 3) + g_up.astype(F32) + g_down.astype(F32)
    up_grad = part(du_all, 3) + u_up.astype(F32) + u_down.astype(F32)
    return input_grad, gate_grad.astype(BF), up_grad.astype(BF)


def solution(mesh):
    torus = Mesh(mesh.devices.reshape(2, 8, 2, 4, 2), AXES)
    rows, hidden = ("yl", "x", "c"), ("yh", "z")
    spread = P(rows + hidden, None)
    both = P(rows, hidden)
    return jax.shard_map(
        on_device,
        mesh=torus,
        in_specs=(spread, both, both, both, both, both),
        out_specs=(spread, both, both),
        check_vma=False,
    )
```
